32 devices in a mesh: rows: 8 (over z, x), cols: 4 (over y, core).
Axes of the slice: x: 2, y: 2, z: 4, core: 2. Of those that a mesh axis runs over, the one named last changes fastest.
Arguments:
- basis: float32 [8192, 4096], P('rows', 'cols'), may hold values from -119.66257 to 119.66257, as said below
- block: float32 [8192, 512], P('rows', 'cols'), may hold values from -1800 to 1800
Outputs:
- ortho: float32 [8192, 512], P('rows', 'cols')
- factors: float32 [4, 128, 128], P('cols')
The draws below stay inside these ranges and needn't reach their ends.
Inputs may be any that keep to these rules, and one draw needn't show every extreme that they name: Under the inner product (sum over rows divided by 8192) the basis columns have squared norms between 0.6 and 1.9, and inner products of distinct basis columns are at most 0.05 in magnitude.
All inputs are finite; a program needn't handle non-finite values.
Results may differ from the reference program's by a relative error of at most 0.000076.
Values sent between devices are 32-bit elements; how exact they have to be, the bound alone decides.
A program may use at most 64 MiB of HBM per device.

```python
import math
import jax
import jax.numpy as jnp
from jax import lax

K = 4096
BLK = 128
NBLK = 4
M = 8192


def draw_basis(key, part):
    keys = jax.random.split(key, 8)
    group = 128
    chosen = jax.random.permutation(keys[0], M)[:K]
    field = (jnp.arange(M, dtype=jnp.int32)[:, None] == chosen[None, :]).astype(jnp.float32)
    for section in range(3):
        order = jax.random.permutation(keys[1 + section], M)
        field = field[order]
        raw = jax.random.normal(keys[4 + section], (M // group, group, group), jnp.float32)
        rotation, upper = jnp.linalg.qr(raw)
        field = jnp.einsum('gij,gjk->gik', rotation, field.reshape(M // group, group, K), precision=lax.Precision.HIGHEST).reshape(M, K)
    lowest = 0.8
    column_scale = jnp.exp(jax.random.uniform(keys[7], (1, K), jnp.float32, math.log(lowest), -math.log(lowest)))
    tilt = min(0.0015 * math.sqrt(M), 0.4)
    drift = jax.random.truncated_normal(jax.random.fold_in(key, 11), -4.0, 4.0, (M, K), jnp.float32)
    return field * math.sqrt(M) * column_scale + tilt * drift


def draw_block(key, part):
    keys = jax.random.split(key, 2)
    normal_part = jax.random.truncated_normal(keys[0], -4.0, 4.0, (M, NBLK * BLK), jnp.float32)
    position = jnp.arange(M, dtype=jnp.float32) / M
    row_scale = jnp.exp(math.log(3.0) * position + math.log(10.0) * jax.random.uniform(keys[1], (M,), jnp.float32))
    return normal_part * row_scale[:, None]


def setup_inputs(seed: int = 0) -> dict:
    key_list = jax.random.split(jax.random.key(seed), 3)
    return {
        "basis": draw_basis(jax.random.fold_in(key_list[2], 71), 0),
        "block": draw_block(jax.random.fold_in(key_list[2], 71), 0),
    }


def solve_block(lower_factor, vectors):
    return jax.scipy.linalg.solve_triangular(lower_factor, vectors, lower=True)

def reference(basis, block):
    highest = lax.Precision.HIGHEST
    coef_one = jnp.dot(basis.T.astype(jnp.float32), block.astype(jnp.float32), precision=highest, preferred_element_type=jnp.float32) / M
    first = block - jnp.dot(basis.astype(jnp.float32), coef_one.astype(jnp.float32), precision=highest, preferred_element_type=jnp.float32)
    coef_two = jnp.dot(basis.T.astype(jnp.float32), first.astype(jnp.float32), precision=highest, preferred_element_type=jnp.float32) / M
    second = first - jnp.dot(basis.astype(jnp.float32), coef_two.astype(jnp.float32), precision=highest, preferred_element_type=jnp.float32)
    pieces = second.reshape(M, NBLK, BLK)
    gram = jnp.einsum('mbi,mbj->bij', pieces, pieces, precision=highest) / M
    lower_factor = jnp.linalg.cholesky(gram)
    solved = jax.vmap(solve_block)(lower_factor, jnp.transpose(pieces, (1, 2, 0)))
    ortho = jnp.transpose(solved, (2, 0, 1)).reshape(M, NBLK * BLK)
    return (ortho, jnp.transpose(lower_factor, (0, 2, 1)))
```

```python
import functools

import jax
import jax.numpy as jnp
from jax import lax
from jax.experimental import pallas as pl
from jax.experimental.pallas import tpu as pltpu
from jax.sharding import PartitionSpec as P

BLK = 128
PIECES = 4
MESH = pl.DeviceIdType.MESH
F32 = jnp.float32


def greet(axis, others):
    barrier = pltpu.get_barrier_semaphore()
    for other in others:
        pl.semaphore_signal(barrier, inc=1, device_id={axis: other}, device_id_type=MESH)
    pl.semaphore_wait(barrier, len(others))


def send(axis, device, source, target, send_sem, recv_sem):
    return pltpu.make_async_remote_copy(
        src_ref=source,
        dst_ref=target,
        send_sem=send_sem,
        recv_sem=recv_sem,
        device_id={axis: device},
        device_id_type=MESH,
    )


def partners():
    me = lax.axis_index("cols")
    core, side = lax.rem(me, 2), lax.div(me, 2)
    return me, core, side, side * 2 + 1 - core, (1 - side) * 2 + core


def columns(index, width):
    return pl.ds(pl.multiple_of(index * width, width), width)


def gather_kernel(block, out, send_sem, recv_sem):
    me, core, side, mate, across = partners()
    greet("cols", (mate, across))
    rows, width = block.shape
    step = rows // PIECES
    far, near, passed = [], [], []
    for q in range(PIECES):
        part = pl.ds(q * step, step)
        far.append(send("cols", across, block.at[part], out.at[part, columns(me, width)], send_sem.at[0, q], recv_sem.at[0, q]))
        far[-1].start()
    for q in range(PIECES):
        part = pl.ds(q * step, step)
        near.append(send("cols", mate, block.at[part], out.at[part, columns(me, width)], send_sem.at[1, q], recv_sem.at[1, q]))
        near[-1].start()
    out[:, columns(me, width)] = block[...]
    for q in range(PIECES):
        part = pl.ds(q * step, step)
        far[q].wait_recv()
        held = out.at[part, columns(across, width)]
        passed.append(send("cols", mate, held, held, send_sem.at[2, q], recv_sem.at[2, q]))
        passed[-1].start()
    for q in range(PIECES):
        near[q].wait_recv()
        passed[q].wait_recv()
    for copy in far + near + passed:
        copy.wait_send()


def first_kernel(partial, base, out, near_in, chip, far_in, send_sem, recv_sem):
    me, core, side, mate, across = partners()
    greet("cols", (mate, across))
    half = partial.shape[0] // 2
    step = half // PIECES

    def mine(q):
        return pl.ds(pl.multiple_of(core * half + q * step, step), step)

    def others(q):
        return pl.ds(pl.multiple_of((1 - core) * half + q * step, step), step)

    near, far, back = [], [], []
    for q in range(PIECES):
        near.append(send("cols", mate, partial.at[others(q)], near_in.at[q], send_sem.at[0, q], recv_sem.at[0, q]))
        near[-1].start()
    for q in range(PIECES):
        near[q].wait_recv()
        chip[q] = partial[mine(q)] + near_in[q]
        far.append(send("cols", across, chip.at[q], far_in.at[q], send_sem.at[1, q], recv_sem.at[1, q]))
        far[-1].start()
    for q in range(PIECES):
        far[q].wait_recv()
        out[mine(q)] = base[mine(q)] - (chip[q] + far_in[q])
        held = out.at[mine(q)]
        back.append(send("cols", mate, held, held, send_sem.at[2, q], recv_sem.at[2, q]))
        back[-1].start()
    for q in range(PIECES):
        back[q].wait_recv()
    for copy in near + far + back:
        copy.wait_send()


def second_kernel(partial, first, out, near_in, chip, far_in, send_sem, recv_sem):
    me, core, side, mate, across = partners()
    greet("cols", (mate, across))
    rows, width = out.shape
    step = rows // PIECES
    near, far = {}, []
    for kind, there in enumerate((1 - side, side)):
        for q in range(PIECES):
            part = pl.ds(q * step, step)
            source = partial.at[part, columns(there * 2 + 1 - core, width)]
            near[kind, q] = send("cols", mate, source, near_in.at[kind, part], send_sem.at[kind, q], recv_sem.at[kind, q])
            near[kind, q].start()
    for q in range(PIECES):
        part = pl.ds(q * step, step)
        near[0, q].wait_recv()
        chip[part] = partial[part, columns(across, width)] + near_in[0, part]
        far.append(send("cols", across, chip.at[part], far_in.at[part], send_sem.at[2, q], recv_sem.at[2, q]))
        far[-1].start()
    for q in range(PIECES):
        part = pl.ds(q * step, step)
        near[1, q].wait_recv()
        own = partial[part, columns(me, width)] + near_in[1, part]
        far[q].wait_recv()
        out[part] = first[part, columns(me, width)] - (own + far_in[part])
    for copy in list(near.values()) + far:
        copy.wait_send()


def ring_kernel(n, streams, work, out, slots, send_sem, recv_sem):
    me = lax.axis_index("rows")
    odd = lax.rem(me, 2)
    place = (1 - odd) * lax.div(me, 2) + odd * (n - 1 - lax.div(me, 2))

    def device(position):
        late = lax.div(position, n // 2)
        return (1 - late) * 2 * position + late * (2 * (n - 1 - position) + 1)

    up = device(lax.rem(place + 1, n))
    down = device(lax.rem(place + n - 1, n))
    greet("rows", (up, down))
    cuts = work.shape[1] // slots.shape[2]
    lane_blocks = streams // cuts
    width, tall = work.shape[2] // lane_blocks, slots.shape[2]

    def target(stream):
        return up if stream < streams // 2 else down

    def chunk(stream, step):
        sign = -1 if stream < streams // 2 else 1
        return lax.rem(place + sign * step + 2 * n, n)

    def lanes(stream):
        return pl.ds(stream // cuts * width, width)

    def band(stream):
        return pl.ds(stream % cuts * tall, tall)

    def reducing(stream, step, source):
        return send("rows", target(stream), source, slots.at[stream, step], send_sem.at[0, stream, step], recv_sem.at[0, stream, step])

    def sharing(stream, step):
        held = out.at[chunk(stream, step - 1), band(stream), lanes(stream)]
        return send("rows", target(stream), held, held, send_sem.at[1, stream, step], recv_sem.at[1, stream, step])

    for stream in range(streams):
        reducing(stream, 0, work.at[chunk(stream, 0), band(stream), lanes(stream)]).start()

    def reduce_step(step, carry):
        for stream in range(streams):
            slot = slots.at[stream, step - 1]
            reducing(stream, step - 1, slot).wait_recv()
            slot[...] = slot[...] + work[chunk(stream, step), band(stream), lanes(stream)]
            reducing(stream, step, slot).start()
        return carry

    lax.fori_loop(1, n - 1, reduce_step, 0)
    for stream in range(streams):
        reducing(stream, n - 2, slots.at[stream, n - 2]).wait_recv()
        own = chunk(stream, n - 1)
        out[own, band(stream), lanes(stream)] = slots[stream, n - 2] + work[own, band(stream), lanes(stream)]
        sharing(stream, 0).start()

    def share_step(step, carry):
        for stream in range(streams):
            sharing(stream, step - 1).wait_recv()
            sharing(stream, step).start()
        return carry

    lax.fori_loop(1, n - 1, share_step, 0)
    for stream in range(streams):
        sharing(stream, n - 2).wait_recv()

    def drain(step, carry):
        for stream in range(streams):
            reducing(stream, step, slots.at[stream, step]).wait_send()
            sharing(stream, step).wait_send()
        return carry

    lax.fori_loop(0, n - 1, drain, 0)


def gram_kernel(n, work, out, held, send_sem, recv_sem):
    me = lax.axis_index("rows")
    peers = [lax.rem(me + d, n) for d in range(1, n)]
    greet("rows", peers)
    parts, wholes = [], []
    for d, peer in enumerate(peers):
        parts.append(send("rows", peer, work.at[peer], held.at[d], send_sem.at[0, d], recv_sem.at[0, d]))
        parts[-1].start()
    total = work[me]
    for d in range(n - 1):
        parts[d].wait_recv()
        total = total + held[d]
    out[me] = total
    for d, peer in enumerate(peers):
        wholes.append(send("rows", peer, out.at[me], out.at[me], send_sem.at[1, d], recv_sem.at[1, d]))
        wholes[-1].start()
    for copy in wholes:
        copy.wait_recv()
    for copy in parts + wholes:
        copy.wait_send()


def factor_kernel(gram, factor, solved):
    size, tile = gram.shape[1], 8
    lane = lax.broadcasted_iota(jnp.int32, (1, size), 1)
    below = lax.broadcasted_iota(jnp.int32, (tile, size), 0)
    for b in range(gram.shape[0]):
        left = [gram[b, pl.ds(i * tile, tile), :] for i in range(size // tile)]
        right = [
            jnp.where(lax.broadcasted_iota(jnp.int32, (tile, size), 1) == below + i * tile, 1.0, 0.0)
            for i in range(size // tile)
        ]
        for j in range(size):
            at, r = j // tile, j % tile
            row = left[at][r : r + 1, :]
            scale = 1.0 / jnp.sqrt(jnp.broadcast_to(row[:, j : j + 1], (1, size)))
            upper = jnp.where(lane >= j, row * scale, 0.0)
            inner = right[at][r : r + 1, :] * scale
            factor[b, j : j + 1, :] = upper
            solved[b, j : j + 1, :] = inner
            upper, inner = upper * scale, inner * scale
            for i in range(at, size // tile):
                column = jnp.broadcast_to(left[i][:, j : j + 1], (tile, size))
                if i == at:
                    column = jnp.where(below > r, column, 0.0)
                left[i] = left[i] - column * upper
                right[i] = right[i] - column * inner


def call(kernel, key, shape, scratch, counts, *arrays):
    return pl.pallas_call(
        kernel,
        out_shape=jax.ShapeDtypeStruct(shape, F32),
        in_specs=[pl.BlockSpec(memory_space=pltpu.VMEM)] * len(arrays),
        out_specs=pl.BlockSpec(memory_space=pltpu.VMEM),
        scratch_shapes=[pltpu.VMEM(s, F32) for s in scratch]
        + [pltpu.SemaphoreType.DMA(counts), pltpu.SemaphoreType.DMA(counts)],
        compiler_params=pltpu.CompilerParams(
            collective_id=key, has_side_effects=True, vmem_limit_bytes=48 * 1024 * 1024
        ),
    )(*arrays)


def sum_rows(x, key):
    n = lax.axis_size("rows")
    deep = x.reshape(n, x.shape[0] // n, x.shape[1])
    cuts = 2 if deep.shape[1] >= 32 else 1
    streams = x.shape[1] // BLK * cuts
    total = call(
        functools.partial(ring_kernel, n, streams),
        key,
        deep.shape,
        [(streams, n - 1, deep.shape[1] // cuts, BLK)],
        (2, streams, n - 1),
        deep,
    )
    return total.reshape(x.shape)


def body(basis, block):
    highest, high = lax.Precision.HIGHEST, lax.Precision.HIGH
    rows, width = block.shape
    n = lax.axis_size("rows")
    wide = width * lax.axis_size("cols")
    inverse = 1.0 / (rows * n)

    def project(piece):
        return (
            lax.dot_general(
                basis, piece, (((0,), (0,)), ((), ())), precision=high, preferred_element_type=F32
            )
            * inverse
        )

    def expand(coef):
        return jnp.dot(basis, coef, precision=high, preferred_element_type=F32)

    piece = (PIECES, rows // 2 // PIECES, wide)
    gathered = call(gather_kernel, 0, (rows, wide), [], (3, PIECES), block)
    coef_one = sum_rows(project(gathered), 1)
    first = call(first_kernel, 2, (rows, wide), [piece] * 3, (3, PIECES), expand(coef_one), gathered)
    coef_two = sum_rows(project(first), 3)
    second = call(
        second_kernel,
        4,
        (rows, width),
        [(2, rows, width), (rows, width), (rows, width)],
        (3, PIECES),
        expand(coef_two),
        first,
    )
    blocks = width // BLK
    pieces = second.reshape(rows, blocks, BLK)
    gram = jnp.einsum("mbi,mbj->bij", pieces, pieces, precision=highest) * inverse
    deep = gram.reshape(n, blocks * BLK // n, BLK)
    gram = call(functools.partial(gram_kernel, n), 5, deep.shape, [(n - 1,) + deep.shape[1:]], (2, n - 1), deep)
    gram = gram.reshape(blocks, BLK, BLK)
    factors, solved = pl.pallas_call(
        factor_kernel,
        out_shape=[jax.ShapeDtypeStruct(gram.shape, F32)] * 2,
        in_specs=[pl.BlockSpec(memory_space=pltpu.VMEM)],
        out_specs=[pl.BlockSpec(memory_space=pltpu.VMEM)] * 2,
    )(gram)
    ortho = jnp.einsum("mbi,bji->mbj", pieces, solved, precision=highest).reshape(rows, width)
    return (ortho, factors)


def solution(mesh):
    placed = (P("rows", "cols"), P("rows", "cols"))
    return jax.shard_map(
        body,
        mesh=mesh,
        in_specs=placed,
        out_specs=(P("rows", "cols"), P("cols", None, None)),
        check_vma=False,
    )
```

```python
import functools

import jax
import jax.numpy as jnp
from jax import lax
from jax.experimental import pallas as pl
from jax.experimental.pallas import tpu as pltpu
from jax.sharding import PartitionSpec as P

BLK = 128
PIECES = 8
MESH = pl.DeviceIdType.MESH
F32 = jnp.float32


def greet(axis, others):
    barrier = pltpu.get_barrier_semaphore()
    for other in others:
        pl.semaphore_signal(barrier, inc=1, device_id={axis: other}, device_id_type=MESH)
    pl.semaphore_wait(barrier, len(others))


def send(axis, device, source, target, send_sem, recv_sem):
    return pltpu.make_async_remote_copy(
        src_ref=source,
        dst_ref=target,
        send_sem=send_sem,
        recv_sem=recv_sem,
        device_id={axis: device},
        device_id_type=MESH,
    )


def partners():
    me = lax.axis_index("cols")
    core, side = lax.rem(me, 2), lax.div(me, 2)
    return me, core, side, side * 2 + 1 - core, (1 - side) * 2 + core


def columns(index, width):
    return pl.ds(pl.multiple_of(index * width, width), width)


def gather_kernel(block, out, send_sem, recv_sem):
    me, core, side, mate, across = partners()
    greet("cols", (mate, across))
    rows, width = block.shape
    step = rows // PIECES
    far, near, passed = [], [], []
    for q in range(PIECES):
        part = pl.ds(q * step, step)
        far.append(send("cols", across, block.at[part], out.at[part, columns(me, width)], send_sem.at[0, q], recv_sem.at[0, q]))
        far[-1].start()
    for q in range(PIECES):
        part = pl.ds(q * step, step)
        near.append(send("cols", mate, block.at[part], out.at[part, columns(me, width)], send_sem.at[1, q], recv_sem.at[1, q]))
        near[-1].start()
    out[:, columns(me, width)] = block[...]
    for q in range(PIECES):
        part = pl.ds(q * step, step)
        far[q].wait_recv()
        held = out.at[part, columns(across, width)]
        passed.append(send("cols", mate, held, held, send_sem.at[2, q], recv_sem.at[2, q]))
        passed[-1].start()
    for q in range(PIECES):
        near[q].wait_recv()
        passed[q].wait_recv()
    for copy in far + near + passed:
        copy.wait_send()


def first_kernel(partial, base, out, own, near_in, chip, far_in, send_sem, recv_sem):
    me, core, side, mate, across = partners()
    greet("cols", (mate, across))
    half = partial.shape[0] // 2
    step = half // PIECES

    def mine(q):
        return pl.ds(pl.multiple_of(core * half + q * step, step), step)

    def others(q):
        return pl.ds(pl.multiple_of((1 - core) * half + q * step, step), step)

    near, far, back = [], [], []
    for q in range(PIECES):
        near.append(send("cols", mate, partial.at[others(q)], near_in.at[q], send_sem.at[0, q], recv_sem.at[0, q]))
        near[-1].start()
    for q in range(PIECES):
        near[q].wait_recv()
        chip[q] = partial[mine(q)] + near_in[q]
        far.append(send("cols", across, chip.at[q], far_in.at[q], send_sem.at[1, q], recv_sem.at[1, q]))
        far[-1].start()
    for q in range(PIECES):
        far[q].wait_recv()
        out[mine(q)] = base[mine(q)] - (chip[q] + far_in[q])
        own[mine(q)] = out[mine(q), columns(me, own.shape[1])]
        held = out.at[mine(q)]
        back.append(send("cols", mate, held, held, send_sem.at[2, q], recv_sem.at[2, q]))
        back[-1].start()
    for q in range(PIECES):
        back[q].wait_recv()
        own[others(q)] = out[others(q), columns(me, own.shape[1])]
    for copy in near + far + back:
        copy.wait_send()


def second_kernel(partial, first, out, near_in, chip, far_in, send_sem, recv_sem):
    me, core, side, mate, across = partners()
    greet("cols", (mate, across))
    rows, width = out.shape
    step = rows // PIECES
    near, far = {}, []
    for kind, there in enumerate((1 - side, side)):
        for q in range(PIECES):
            part = pl.ds(q * step, step)
            source = partial.at[part, columns(there * 2 + 1 - core, width)]
            near[kind, q] = send("cols", mate, source, near_in.at[kind, part], send_sem.at[kind, q], recv_sem.at[kind, q])
            near[kind, q].start()
    for q in range(PIECES):
        part = pl.ds(q * step, step)
        near[0, q].wait_recv()
        chip[part] = partial[part, columns(across, width)] + near_in[0, part]
        far.append(send("cols", across, chip.at[part], far_in.at[part], send_sem.at[2, q], recv_sem.at[2, q]))
        far[-1].start()
    for q in range(PIECES):
        part = pl.ds(q * step, step)
        near[1, q].wait_recv()
        own = partial[part, columns(me, width)] + near_in[1, part]
        far[q].wait_recv()
        out[part] = first[part] - (own + far_in[part])
    for copy in list(near.values()) + far:
        copy.wait_send()


def ring_kernel(n, work, out, slots, send_sem, recv_sem):
    me = lax.axis_index("rows")
    odd = lax.rem(me, 2)
    place = (1 - odd) * lax.div(me, 2) + odd * (n - 1 - lax.div(me, 2))

    def device(position):
        late = lax.div(position, n // 2)
        return (1 - late) * 2 * position + late * (2 * (n - 1 - position) + 1)

    up = device(lax.rem(place + 1, n))
    down = device(lax.rem(place + n - 1, n))
    greet("rows", (up, down))
    streams, tall = slots.shape[0], slots.shape[2]
    lane_blocks = streams // 4

    def sign(stream):
        return 1 - 2 * (stream % 2)

    def band(stream):
        return stream // 2 // lane_blocks

    def reach(stream):
        return n // 2 - (stream % 2 + band(stream)) % 2

    def place_of(stream):
        return pl.ds(band(stream) * tall, tall), pl.ds(stream // 2 % lane_blocks * BLK, BLK)

    def chunk(offset):
        return lax.rem(place + offset + 2 * n, n)

    def move(phase, stream, step, source, target):
        device_id = up if stream % 2 == 0 else down
        return send("rows", device_id, source, target, send_sem.at[phase, stream, step], recv_sem.at[phase, stream, step])

    def reducing(stream, step, source=None):
        slot = slots.at[stream, step]
        return move(0, stream, step, slot if source is None else source, slot)

    def sharing(stream, step):
        held = out.at[(chunk(-sign(stream) * step), *place_of(stream))]
        return move(1, stream, step, held, held)

    def reduce_one(stream, step):
        slot = slots.at[stream, step - 1]
        reducing(stream, step - 1).wait_recv()
        slot[...] = slot[...] + work[(chunk(sign(stream) * (reach(stream) - step)), *place_of(stream))]
        reducing(stream, step, slot).start()

    def share_one(stream, step):
        sharing(stream, step - 1).wait_recv()
        sharing(stream, step).start()

    def drain_one(stream, step):
        reducing(stream, step).wait_send()
        sharing(stream, step).wait_send()

    every = range(streams)
    longer = [stream for stream in every if reach(stream) == n // 2]

    def sweep(one, begin):
        def each(step, carry):
            for stream in every:
                one(stream, step)
            return carry

        lax.fori_loop(begin, n // 2 - 1, each, 0)
        for stream in longer:
            one(stream, n // 2 - 1)

    for stream in every:
        reducing(stream, 0, work.at[(chunk(sign(stream) * reach(stream)), *place_of(stream))]).start()
    sweep(reduce_one, 1)
    for pair in range(0, streams, 2):
        own = (chunk(0), *place_of(pair))
        total = work[own]
        for stream in (pair, pair + 1):
            reducing(stream, reach(stream) - 1).wait_recv()
            total = total + slots[stream, reach(stream) - 1]
        out[own] = total
        for stream in (pair, pair + 1):
            sharing(stream, 0).start()
    sweep(share_one, 1)
    for stream in every:
        sharing(stream, reach(stream) - 1).wait_recv()
    sweep(drain_one, 0)


def gram_kernel(n, work, out, held, send_sem, recv_sem):
    me = lax.axis_index("rows")
    peers = [lax.rem(me + d, n) for d in range(1, n)]
    greet("rows", peers)
    parts, wholes = [], []
    for d, peer in enumerate(peers):
        parts.append(send("rows", peer, work.at[peer], held.at[d], send_sem.at[0, d], recv_sem.at[0, d]))
        parts[-1].start()
    total = work[me]
    for d in range(n - 1):
        parts[d].wait_recv()
        total = total + held[d]
    out[me] = total
    for d, peer in enumerate(peers):
        wholes.append(send("rows", peer, out.at[me], out.at[me], send_sem.at[1, d], recv_sem.at[1, d]))
        wholes[-1].start()
    for copy in wholes:
        copy.wait_recv()
    for copy in parts + wholes:
        copy.wait_send()


def factor_kernel(gram, factor, solved):
    size, tile = gram.shape[1], 8
    lane = lax.broadcasted_iota(jnp.int32, (1, size), 1)
    below = lax.broadcasted_iota(jnp.int32, (tile, size), 0)
    for b in range(gram.shape[0]):
        left = [gram[b, pl.ds(i * tile, tile), :] for i in range(size // tile)]
        right = [
            jnp.where(lax.broadcasted_iota(jnp.int32, (tile, size), 1) == below + i * tile, 1.0, 0.0)
            for i in range(size // tile)
        ]
        for j in range(size):
            at, r = j // tile, j % tile
            row = left[at][r : r + 1, :]
            scale = 1.0 / jnp.sqrt(jnp.broadcast_to(row[:, j : j + 1], (1, size)))
            upper = jnp.where(lane >= j, row * scale, 0.0)
            inner = right[at][r : r + 1, :] * scale
            factor[b, j : j + 1, :] = upper
            solved[b, j : j + 1, :] = inner
            upper, inner = upper * scale, inner * scale
            for i in range(at, size // tile):
                column = jnp.broadcast_to(left[i][:, j : j + 1], (tile, size))
                if i == at:
                    column = jnp.where(below > r, column, 0.0)
                left[i] = left[i] - column * upper
                right[i] = right[i] - column * inner


def call(kernel, key, shape, scratch, counts, *arrays):
    return pl.pallas_call(
        kernel,
        out_shape=jax.tree.map(lambda s: jax.ShapeDtypeStruct(s, F32), shape, is_leaf=lambda s: isinstance(s[0], int)),
        in_specs=[pl.BlockSpec(memory_space=pltpu.VMEM)] * len(arrays),
        out_specs=jax.tree.map(
            lambda s: pl.BlockSpec(memory_space=pltpu.VMEM), shape, is_leaf=lambda s: isinstance(s[0], int)
        ),
        scratch_shapes=[pltpu.VMEM(s, F32) for s in scratch]
        + [pltpu.SemaphoreType.DMA(counts), pltpu.SemaphoreType.DMA(counts)],
        compiler_params=pltpu.CompilerParams(
            collective_id=key, has_side_effects=True, vmem_limit_bytes=16 * 1024 * 1024
        ),
    )(*arrays)


def sum_rows(x, key):
    n = lax.axis_size("rows")
    deep = x.reshape(n, x.shape[0] // n, x.shape[1])
    streams = 4 * (x.shape[1] // BLK)
    total = call(
        functools.partial(ring_kernel, n),
        key,
        deep.shape,
        [(streams, n // 2, deep.shape[1] // 2, BLK)],
        (2, streams, n // 2),
        deep,
    )
    return total.reshape(x.shape)


def body(basis, block):
    highest, high = lax.Precision.HIGHEST, lax.Precision.HIGH
    rows, width = block.shape
    n = lax.axis_size("rows")
    wide = width * lax.axis_size("cols")
    inverse = 1.0 / (rows * n)

    def project(piece):
        return (
            lax.dot_general(
                basis, piece, (((0,), (0,)), ((), ())), precision=high, preferred_element_type=F32
            )
            * inverse
        )

    def expand(coef):
        return jnp.dot(basis, coef, precision=high, preferred_element_type=F32)

    piece = (PIECES, rows // 2 // PIECES, wide)
    gathered = call(gather_kernel, 0, (rows, wide), [], (3, PIECES), block)
    coef_one = sum_rows(project(gathered), 1)
    first, own = call(first_kernel, 2, [(rows, wide), (rows, width)], [piece] * 3, (3, PIECES), expand(coef_one), gathered)
    coef_two = sum_rows(project(first), 3)
    second = call(
        second_kernel,
        4,
        (rows, width),
        [(2, rows, width), (rows, width), (rows, width)],
        (3, PIECES),
        expand(coef_two),
        own,
    )
    blocks = width // BLK
    pieces = second.reshape(rows, blocks, BLK)
    gram = jnp.einsum("mbi,mbj->bij", pieces, pieces, precision=highest) * inverse
    deep = gram.reshape(n, blocks * BLK // n, BLK)
    gram = call(functools.partial(gram_kernel, n), 5, deep.shape, [(n - 1,) + deep.shape[1:]], (2, n - 1), deep)
    gram = gram.reshape(blocks, BLK, BLK)
    factors, solved = pl.pallas_call(
        factor_kernel,
        out_shape=[jax.ShapeDtypeStruct(gram.shape, F32)] * 2,
        in_specs=[pl.BlockSpec(memory_space=pltpu.VMEM)],
        out_specs=[pl.BlockSpec(memory_space=pltpu.VMEM)] * 2,
    )(gram)
    ortho = jnp.einsum("mbi,bji->mbj", pieces, solved, precision=highest).reshape(rows, width)
    return (ortho, factors)


def solution(mesh):
    placed = (P("rows", "cols"), P("rows", "cols"))
    return jax.shard_map(
        body,
        mesh=mesh,
        in_specs=placed,
        out_specs=(P("rows", "cols"), P("cols", None, None)),
        check_vma=False,
    )
```
